256 devices in a mesh: group: 4 (over x), shard: 64 (over y, z, core).
Axes of the slice: x: 4, y: 4, z: 8, core: 2. Of those that a mesh axis runs over, the one named last changes fastest.
Arguments:
- table: bfloat16 [2, 524288, 128], P(None, 'shard'), may hold values from -3 to 3
- owners: int32 [4, 2, 2, 32768, 1], P('group', None, None, 'shard'), may hold values from 0 to 63; in each aligned block of 512 rows (0 to 511, 512 to 1023, ..., all dimensions but the last counted through in order) at most 24 rows name the same one
- offsets: int32 [4, 2, 2, 32768], P('group', None, None, 'shard'), may hold values from 0 to 8191
- bag_lengths: int32 [4, 2, 2, 64, 128], P('group', None, None, 'shard'), may hold values from 1 to 16, 512 in all within a row
- dense_feats: float32 [4, 2, 8192, 13], P('group', None, 'shard'), may hold values from -6 to 6
- labels: int32 [4, 2, 8192], P('group', None, 'shard'), may hold values 0 or 1
- bottom_weight: float32 [13, 128], replicated, may hold values from -1.75 to 1.75
- top_weight: float32 [384, 1024], P('shard'), may hold values from -0.3125 to 0.3125
- out_weight: float32 [1024], replicated, may hold values from -1 to 1
- client_group: int32 [16], replicated, may hold values from 0 to 3
Outputs:
- emb_delta: float32 [2, 524288, 128], P(None, 'shard')
- top_delta: float32 [384, 1024], P('shard')
- bottom_delta: float32 [13, 128], replicated
- out_delta: float32 [1024], replicated
The draws below stay inside these ranges and needn't reach their ends.
Inputs may be any that keep to these rules, and one draw needn't show every extreme that they name: `owners`: in each device's block of 512 lookups of one group, step and table, no owner is named by more than 24 lookups. `bag_lengths`: the 128 bag sizes of one device, group, step and table sum to 512.
All inputs are finite; a program needn't handle non-finite values. No bound on the sum of `labels` on one device may be relied on, other than what follows from the above.
Results may differ from the reference program's by a relative error of at most 0.008.
Values may be sent and summed in bfloat16 or wider, within the bound.
No kernel may reach another device: no remote copies, remote signals or barrier semaphores. Data moves between devices by JAX's collectives and lax.ppermute only.
A program may use at most 128 MiB of HBM per device.

```python
import math
from functools import partial
import jax
import jax.numpy as jnp
import numpy as np
from jax import lax

NTAB = 2
ROWS_DEV = 8192
EMB = 128
DENSE = 13
HID = 1024
STEPS = 2
B_DEV = 128
BAGMAX = 16
CLIENTS = 16
ROWS = 524288
BATCH = 8192
LOOK_DEV = 512
LOOKUPS = 32768
CAP = 24
ZW = 384
N_GROUP = 4
N_SHARD = 64


def place_ends(values, key, smallest, top_value):
    dims = values.shape
    index_at = [jax.random.randint(jax.random.fold_in(key, axis), (), 0, dims[axis]) for axis in range(len(dims))]
    values = values.at[tuple(index_at)].set(smallest)
    longest = dims.index(max(dims))
    index_at[longest] = (index_at[longest] + 1) % dims[longest]
    return values.at[tuple(index_at)].set(top_value)


def steps_of(rng, shape, pieces, least, high):
    factor_of, own = 1.0, jax.random.fold_in(rng, 6)
    for dim, blocks in pieces:
        steps = jnp.exp(jax.random.uniform(jax.random.fold_in(own, dim), (blocks,), jnp.float32, least / len(pieces), high / len(pieces)))
        factor_of = factor_of * jnp.repeat(steps, shape[dim] // blocks).reshape([-1 if axis == dim else 1 for axis in range(len(shape))])
    return factor_of


def split_up(number_of, total, limit, lean):
    weights = [(1 << 20) // math.isqrt(grade ** lean) + 1 for grade in range(2, number_of + 1)]
    surplus, holding = total - limit - (number_of - 1), [1] * (number_of - 1)
    while surplus > 0:
        movable = [i for i in range(number_of - 1) if holding[i] < limit]
        mass, left = sum([weights[i] for i in movable]), surplus
        for i in movable:
            extra = min(limit - holding[i], max(1, left * weights[i] // mass), surplus)
            holding[i] = holding[i] + extra
            surplus = surplus - extra
    return np.array([limit] + holding)


def ragged_sizes(own_key, number_of, total, reach, skew):
    if number_of == 2:
        one = jax.random.randint(own_key, (), max(1, total - reach), min(reach, total - 1) + 1)
        return jnp.stack([one, total - one])
    tallies = jnp.asarray(split_up(number_of, total, reach, skew), jnp.int32)
    couples = (number_of - 1) // 2
    giver, taker = tallies[1:1 + 2 * couples:2], tallies[2:2 + 2 * couples:2]
    room = jnp.minimum(giver - 1, reach - taker)
    passed = jax.random.randint(jax.random.fold_in(own_key, 1), (couples,), 0, 1 << 20) % (room + 1)
    tallies = tallies.at[1:1 + 2 * couples:2].set(giver - passed).at[2:2 + 2 * couples:2].set(taker + passed)
    return tallies[jax.random.permutation(jax.random.fold_in(own_key, 2), number_of)]


def deal_out(rng, own, number, rows, number_of, top, reach, lean):
    sequence = jax.random.permutation(rng, number_of)
    packed, ordinary = load_shares(number_of, rows * top, reach, lean, True), load_shares(number_of, rows * top, reach, lean, False)
    places = jnp.arange(number_of)

    def named(tallies, turn):
        used = int((tallies > 0).sum())
        fixed = max(1, used // 4)
        moved = fixed + (places - fixed + turn * (used - fixed)) % max(1, number_of - fixed)
        return jnp.zeros((number_of,), jnp.int32).at[sequence[jnp.where(places < fixed, places, moved)]].set(jnp.asarray(tallies, jnp.int32))

    tallies = jnp.where(number % 4 == 0, named(packed, number // 4), named(ordinary, number - number // 4 - 1))
    mixed = jax.random.permutation(jax.random.fold_in(own, 3), number_of)
    giver, receiver = mixed[0:number_of // 2 * 2:2], mixed[1:number_of // 2 * 2:2]
    room = jnp.minimum(tallies[giver] - 1, reach - tallies[receiver]) // 2
    room = jnp.where((giver == sequence[0]) | (receiver == sequence[0]) | (tallies[receiver] == 0), 0, jnp.maximum(room, 0))
    moved = jax.random.randint(jax.random.fold_in(own, 4), (number_of // 2,), 0, 1 << 20) % (room + 1)
    tallies = tallies.at[giver].add(-moved).at[receiver].add(moved)
    items = jnp.searchsorted(jnp.cumsum(tallies), jnp.arange(rows * top), side="right").astype(jnp.int32)
    table = items.reshape(top, rows).T
    table = table[jax.random.permutation(jax.random.fold_in(own, 1), rows)]
    turn = jax.random.randint(jax.random.fold_in(own, 2), (rows, 1), 0, top)
    return jnp.take_along_axis(table, (jnp.arange(top)[None, :] + turn) % top, axis=1)


def load_shares(amount, total, most, skew, full):
    portions = [(1 << 20) // math.isqrt(standing ** skew) + 1 for standing in range(1, amount + 1)]
    largest = most if full else min(most, max(-(-total // amount), total * portions[0] // sum(portions)))
    least = 1 if total - largest >= amount - 1 else 0
    given, spare = [largest] + [least] * (amount - 1), total - largest - least * (amount - 1)
    while spare > 0:
        free = [i for i in range(1, amount) if given[i] < largest] or [i for i in range(1, amount) if given[i] < most]
        mass, remaining = sum([portions[i] for i in free]), spare
        for i in free:
            addition = min(most - given[i], max(1, remaining * portions[i] // mass), spare)
            given[i] = given[i] + addition
            spare = spare - addition
    return np.array(given)


def normal_values(key, extent, width, most, pieces=(), kind=jnp.bfloat16):
    values = width * jax.random.normal(key, extent, jnp.float32)
    if pieces:
        values = values * steps_of(key, extent, pieces, -0.22, 0.18)
    return jnp.clip(values, -most, most).astype(kind)


def setup_inputs(seed: int = 0) -> dict:
    key_of = jax.random.split(jax.random.key(seed), 11)
    table = normal_values(key_of[0], (NTAB, ROWS, EMB), 0.5, 3.0, ((1, 64),))
    owners_keys = jax.random.split(jax.random.fold_in(key_of[1], 1), N_GROUP * STEPS * NTAB * LOOKUPS // LOOK_DEV)
    owners_turns = jax.random.permutation(jax.random.fold_in(key_of[1], 3), N_GROUP * STEPS * NTAB * LOOKUPS // LOOK_DEV)
    owners = jax.vmap(lambda own, number: deal_out(jax.random.fold_in(key_of[1], 2), own, number, LOOK_DEV, N_SHARD, 1, CAP, 2))(owners_keys, owners_turns).reshape((N_GROUP, STEPS, NTAB, LOOKUPS, 1))
    offsets = place_ends(jax.random.randint(key_of[2], (N_GROUP, STEPS, NTAB, LOOKUPS), 0, ROWS_DEV), jax.random.fold_in(key_of[2], 1), 0, ROWS_DEV - 1).astype(jnp.int32)
    bag_lengths = jax.vmap(lambda own: ragged_sizes(own, B_DEV, LOOK_DEV, BAGMAX, 1))(jax.random.split(key_of[3], N_GROUP * STEPS * NTAB * N_SHARD)).reshape((N_GROUP, STEPS, NTAB, N_SHARD, B_DEV)).astype(jnp.int32)
    dense_feats = normal_values(key_of[4], (N_GROUP, STEPS, BATCH, DENSE), 1.0, 6.0, ((0, 4), (2, 64)), jnp.float32)
    labels = place_ends((jax.random.randint(key_of[5], (N_GROUP, STEPS, BATCH), 0, 2) < 1).astype(jnp.int32), jax.random.fold_in(key_of[5], 1), 0, 1)
    bottom_weight = normal_values(key_of[6], (DENSE, EMB), DENSE ** -0.5, 1.75, (), jnp.float32)
    top_weight = normal_values(key_of[7], (ZW, HID), ZW ** -0.5, 0.3125, ((0, 64),), jnp.float32)
    out_weight = normal_values(key_of[8], (HID,), 32 ** -0.5, 1.0, (), jnp.float32)
    client_group = place_ends(jax.random.randint(key_of[9], (CLIENTS,), 0, N_GROUP), jax.random.fold_in(key_of[9], 1), 0, N_GROUP - 1).astype(jnp.int32)
    return dict(table=table, owners=owners, offsets=offsets, bag_lengths=bag_lengths, dense_feats=dense_feats, labels=labels, bottom_weight=bottom_weight, top_weight=top_weight, out_weight=out_weight, client_group=client_group)


emb_rate = 2.0
dense_rate = 0.5
highest = lax.Precision.HIGHEST


def bag_index(lengths, count):
    bounds = jnp.cumsum(lengths)[:-1].astype(jnp.int32)
    marker = jnp.zeros((count,), jnp.int32).at[bounds].add(1)
    return jnp.cumsum(marker).astype(jnp.int32)


def smooth_slope(value):
    gate = jax.nn.sigmoid(value)
    return gate * (1.0 + value * (1.0 - gate))


def reference(table, owners, offsets, bag_lengths, dense_feats, labels, bottom_weight, top_weight, out_weight, client_group):
    indexer = partial(bag_index, count=LOOK_DEV)
    members = jax.vmap(jax.vmap(jax.vmap(jax.vmap(indexer))))(bag_lengths)
    members = members + (jnp.arange(N_SHARD, dtype=jnp.int32) * B_DEV)[:, None]
    members = members.reshape(N_GROUP, STEPS, NTAB, LOOKUPS).astype(jnp.int32)
    all_rows = (owners[..., 0] * ROWS_DEV + offsets).astype(jnp.int32)
    emb_total = jnp.zeros((NTAB, ROWS, EMB), jnp.float32)
    top_total = jnp.zeros((ZW, HID), jnp.float32)
    bottom_total = jnp.zeros((DENSE, EMB), jnp.float32)
    out_total = jnp.zeros((HID,), jnp.float32)
    for group in range(N_GROUP):
        weight = jnp.sum((client_group == group).astype(jnp.float32)) * N_GROUP / CLIENTS
        delta = jnp.zeros((NTAB, ROWS, EMB), jnp.float32)
        w_bottom, w_top, w_out = bottom_weight, top_weight, out_weight
        for step in range(STEPS):
            pooled = []
            for which in range(NTAB):
                wanted = all_rows[group, step, which]
                fetched = (table[which][wanted].astype(jnp.float32) + delta[which][wanted]).astype(jnp.bfloat16)
                pooled.append(jax.ops.segment_sum(fetched.astype(jnp.float32), members[group, step, which], num_segments=BATCH))
            feats = dense_feats[group, step]
            target = labels[group, step].astype(jnp.float32)
            bpre = jnp.dot(feats, w_bottom, precision=highest)
            bottom = jax.nn.silu(bpre)
            joined = jnp.concatenate([bottom] + pooled, 1).astype(jnp.bfloat16)
            top_low = w_top.astype(jnp.bfloat16)
            pre = jnp.dot(joined, top_low, preferred_element_type=jnp.float32)
            hidden = jax.nn.silu(pre)
            logit = jnp.dot(hidden, w_out, precision=highest)
            dlogit = jax.nn.sigmoid(logit) - target
            dpre = (dlogit[:, None] * w_out[None, :] * smooth_slope(pre)).astype(jnp.bfloat16)
            dz = jnp.dot(dpre, top_low.T, preferred_element_type=jnp.float32)
            for which in range(NTAB):
                dpooled = dz[:, EMB * (which + 1):EMB * (which + 2)].astype(jnp.bfloat16)
                grads = dpooled[members[group, step, which]].astype(jnp.float32)
                delta = delta.at[which, all_rows[group, step, which]].add(-emb_rate * grads)
            grad_top = jnp.dot(joined.T, dpre, preferred_element_type=jnp.float32) / BATCH
            dbottom = dz[:, :EMB] * smooth_slope(bpre)
            grad_bottom = jnp.dot(feats.T, dbottom, precision=highest) / BATCH
            grad_out = jnp.dot(hidden.T, dlogit, precision=highest) / BATCH
            w_top = w_top - dense_rate * grad_top
            w_bottom = w_bottom - dense_rate * grad_bottom
            w_out = w_out - dense_rate * grad_out
        rounded = lax.optimization_barrier((weight * delta).astype(jnp.bfloat16))
        emb_total = emb_total + rounded.astype(jnp.float32)
        top_total = top_total + weight * (w_top - top_weight)
        bottom_total = bottom_total + weight * (w_bottom - bottom_weight)
        out_total = out_total + weight * (w_out - out_weight)
    return emb_total, top_total, bottom_total, out_total
```

```python
import jax
import jax.numpy as jnp
from jax import lax
from jax.experimental import pallas as pl
from jax.experimental.pallas import tpu as pltpu
from jax.sharding import PartitionSpec as P

emb_rate = 2.0
dense_rate = 0.5
bf16 = jnp.bfloat16
f32 = jnp.float32
i32 = jnp.int32

NS = 64
NG = 4
ZS, YS = 8, 4
CAP = 24
SLOTS = 2 * CAP
LOOKS = 512
SAMPLES = 128
EMB = 128
ROWS = 8192
HID = 1024
DENSE = 13
ALL_SLOTS = NS * SLOTS
BATCH = NS * SAMPLES

z_groups = [[y * 16 + z * 2 + c for z in range(ZS)] for y in range(YS) for c in range(2)]
y_groups = [[y * 16 + z * 2 + c for y in range(YS)] for z in range(ZS) for c in range(2)]


def params(mb=48):
    return pltpu.CompilerParams(vmem_limit_bytes=mb * 1024 * 1024)


vm = pl.BlockSpec(memory_space=pltpu.VMEM)
sm = pl.BlockSpec(memory_space=pltpu.SMEM)
hb = pl.BlockSpec(memory_space=pl.ANY)


def iota(shape, dim):
    return lax.broadcasted_iota(i32, shape, dim)


def ones_where(mask):
    return jnp.where(mask, 1.0, 0.0).astype(bf16)


def mm(a, b):
    return lax.dot_general(a, b, (((1,), (0,)), ((), ())), preferred_element_type=f32)


def mm_nt(a, b):
    return lax.dot_general(a, b, (((1,), (1,)), ((), ())), preferred_element_type=f32)


def mm_tn(a, b):
    return lax.dot_general(a, b, (((0,), (0,)), ((), ())), preferred_element_type=f32)


def route_kernel(me_ref, own_ref, off_ref, req_ref, slot_ref):
    earlier = ones_where(iota((LOOKS, LOOKS), 0) < iota((LOOKS, LOOKS), 1))
    total = jnp.zeros((NS, 2 * SLOTS), f32)
    count = jnp.zeros((NS, 2 * SLOTS), f32)
    for st in range(4):
        own = own_ref[st : st + 1, :]
        off = off_ref[st : st + 1, :]
        named = iota((NS, LOOKS), 0) == own
        before = mm(ones_where(named), earlier)
        rank = jnp.sum(jnp.where(named, before, 0.0), axis=0, keepdims=True).astype(i32)
        column = ones_where(iota((2 * SLOTS, LOOKS), 0) == rank + st * CAP)
        high = jnp.where(named, (off >> 8).astype(f32), 0.0).astype(bf16)
        low = jnp.where(named, (off & 255).astype(f32), 0.0).astype(bf16)
        total = total + mm_nt(high, column) * 256.0 + mm_nt(low, column)
        count = count + mm_nt(ones_where(named), column)
        slot_ref[st : st + 1, :] = own * SLOTS + (st % 2) * CAP + rank
    spare = me_ref[0] * CAP + iota((NS, 2 * SLOTS), 1) % CAP
    req_ref[...] = jnp.where(count > 0.5, total.astype(i32), spare)


def route(me, own, off):
    return pl.pallas_call(
        route_kernel,
        name="route",
        in_specs=[sm, vm, vm],
        out_specs=[vm, vm],
        out_shape=[
            jax.ShapeDtypeStruct((NS, 2 * SLOTS), i32),
            jax.ShapeDtypeStruct((4, LOOKS), i32),
        ],
        compiler_params=params(),
    )(me, own, off)


def pool_kernel(slot_ref, bag_ref, a_ref, at_ref):
    upto = ones_where(iota((SAMPLES, SAMPLES), 1) <= iota((SAMPLES, SAMPLES), 0))
    below = ones_where(iota((SAMPLES, SAMPLES), 1) < iota((SAMPLES, SAMPLES), 0))
    look = iota((SAMPLES, LOOKS), 1).astype(f32)
    for t in range(2):
        lens = jnp.broadcast_to(bag_ref[t : t + 1, :], (8, SAMPLES)).astype(f32).astype(bf16)
        ends = mm_nt(upto, lens)[:, :1]
        starts = mm_nt(below, lens)[:, :1]
        member = ones_where((look >= starts) & (look < ends))
        slot = slot_ref[t : t + 1, :]
        for q in range(ALL_SLOTS // LOOKS):
            at_slot = ones_where(iota((LOOKS, LOOKS), 0) + q * LOOKS == slot)
            a_ref[t * SAMPLES : (t + 1) * SAMPLES, q * LOOKS : (q + 1) * LOOKS] = mm_nt(
                member, at_slot
            ).astype(bf16)
            at_ref[q * LOOKS : (q + 1) * LOOKS, t * SAMPLES : (t + 1) * SAMPLES] = mm_nt(
                at_slot, member
            ).astype(bf16)


def pool_matrix(slot, bags):
    return pl.pallas_call(
        pool_kernel,
        name="pool_matrix",
        in_specs=[vm, vm],
        out_specs=[vm, vm],
        out_shape=[
            jax.ShapeDtypeStruct((2 * SAMPLES, ALL_SLOTS), bf16),
            jax.ShapeDtypeStruct((ALL_SLOTS, 2 * SAMPLES), bf16),
        ],
        compiler_params=params(),
    )(slot, bags)


def clash_kernel(idx_ref, out_ref):
    idx = idx_ref[...]
    lane = iota(idx.shape, 1)
    clash = jnp.zeros(idx.shape, i32)
    for d in range(1, 8):
        same = (idx == jnp.concatenate([idx[:, -d:], idx[:, :-d]], axis=1)) & (lane % 8 >= d)
        clash = clash | jnp.where(same, 1, 0)
    first = jnp.max(jnp.where(lane < SLOTS, clash, 0), axis=1, keepdims=True)
    second = jnp.max(jnp.where(lane >= SLOTS, clash, 0), axis=1, keepdims=True)
    out_ref[...] = jnp.where(iota((idx.shape[0], 2), 1) == 0, first, second)


def clashes(idx):
    return pl.pallas_call(
        clash_kernel,
        name="clashes",
        in_specs=[vm],
        out_specs=vm,
        out_shape=jax.ShapeDtypeStruct((idx.shape[0], 2), i32),
        compiler_params=params(),
    )(idx)


def gather_rows(idx_ref, first, tables, stage, out_ref):
    def one(s, _):
        base = pl.multiple_of(s * SLOTS, 8)
        for j in range(SLOTS):
            row = idx_ref[s, first + j]
            stage[pl.ds(base + j, 1), :] = tables[j // CAP][pl.ds(row, 1), :]
        return 0

    lax.fori_loop(0, NS, one, 0)
    out_ref[...] = stage[...].astype(bf16)


def add_rows(idx_ref, base_idx, first, clash_ref, step, stage, tables):
    def one(s, _):
        base = pl.multiple_of(s * SLOTS, 8)
        source = base_idx + s
        clear = clash_ref[source, step] == 0

        @pl.when(clear)
        def _():
            for b in range(0, CAP, 8):
                held = []
                for t in range(2):
                    for j in range(8):
                        at = t * CAP + b + j
                        row = idx_ref[source, first + at]
                        held.append((t, row, tables[t][pl.ds(row, 1), :] + stage[pl.ds(base + at, 1), :]))
                for t, row, value in held:
                    tables[t][pl.ds(row, 1), :] = value

        @pl.when(jnp.logical_not(clear))
        def _():
            for at in range(SLOTS):
                table = tables[at // CAP]
                row = idx_ref[source, first + at]
                table[pl.ds(row, 1), :] = table[pl.ds(row, 1), :] + stage[pl.ds(base + at, 1), :]

        return 0

    lax.fori_loop(0, NS, one, 0)


def gather_kernel(idx_ref, tab_ref, out_ref, stage):
    gather_rows(idx_ref, 0, [tab_ref.at[0], tab_ref.at[1]], stage, out_ref)


def gather_first(idx, table32):
    return pl.pallas_call(
        gather_kernel,
        name="gather_first",
        in_specs=[sm, vm],
        out_specs=vm,
        out_shape=jax.ShapeDtypeStruct((ALL_SLOTS, EMB), bf16),
        scratch_shapes=[pltpu.VMEM((ALL_SLOTS, EMB), f32)],
        compiler_params=params(),
    )(idx, table32)


def owner_kernel(idx_ref, clash_ref, grad_ref, tab_ref, out_ref, new0, new1, stage, sems):
    copies = [
        pltpu.make_async_copy(tab_ref.at[t], new, sems.at[t]) for t, new in enumerate((new0, new1))
    ]
    for c in copies:
        c.start()
    stage[...] = grad_ref[...].astype(f32) * -emb_rate
    for c in copies:
        c.wait()
    add_rows(idx_ref, 0, 0, clash_ref, 0, stage, [new0, new1])
    gather_rows(idx_ref, SLOTS, [new0, new1], stage, out_ref)


def owner_step(idx, clash, grads, table32):
    return pl.pallas_call(
        owner_kernel,
        name="owner_step",
        in_specs=[sm, sm, vm, hb],
        out_specs=vm,
        out_shape=jax.ShapeDtypeStruct((ALL_SLOTS, EMB), bf16),
        scratch_shapes=[
            pltpu.VMEM((ROWS, EMB), f32),
            pltpu.VMEM((ROWS, EMB), f32),
            pltpu.VMEM((ALL_SLOTS, EMB), f32),
            pltpu.SemaphoreType.DMA((2,)),
        ],
        compiler_params=params(),
    )(idx, clash, grads, table32)


def make_total_kernel(step):
    def total_kernel(me_ref, weight_ref, idx_ref, clash_ref, *refs):
        refs = list(refs)
        lists = [refs.pop(0) for _ in range(NG)]
        old = refs.pop(0) if step else None
        out_ref = refs.pop(0)
        part, stage, sem, old_sem = refs
        group = me_ref[1]
        if step:
            seed = pltpu.make_async_copy(old, out_ref, old_sem)
            seed.start()
            seed.wait()
        else:
            out_ref[...] = jnp.zeros(out_ref.shape, f32)

        def one(k, _):
            apart = (group + NG - k) % NG
            for d in range(NG):

                @pl.when(apart == d)
                def _(d=d):
                    copy = pltpu.make_async_copy(lists[d], part, sem)
                    copy.start()
                    copy.wait()

            stage[...] = part[...].astype(f32) * weight_ref[k]
            add_rows(
                idx_ref, k * NS, step * SLOTS, clash_ref, step, stage, [out_ref.at[0], out_ref.at[1]]
            )
            return 0

        lax.fori_loop(0, NG, one, 0)

    return total_kernel


def add_lists(me, weights, idx, clash, lists, old, step):
    operands = [me, weights, idx, clash, *lists] + ([old] if step else [])
    return pl.pallas_call(
        make_total_kernel(step),
        name="add_lists_%d" % step,
        in_specs=[sm, sm, sm, sm] + [hb] * (len(operands) - 4),
        out_specs=vm,
        out_shape=jax.ShapeDtypeStruct((2, ROWS, EMB), f32),
        scratch_shapes=[
            pltpu.VMEM((ALL_SLOTS, EMB), bf16),
            pltpu.VMEM((ALL_SLOTS, EMB), f32),
            pltpu.SemaphoreType.DMA,
            pltpu.SemaphoreType.DMA,
        ],
        compiler_params=params(),
    )(*operands)


def top_pick(core):
    row = iota((384, 256), 1)
    device = 2 * (row // 8) + core
    inside = row % 8
    return ones_where((inside < 6) & (device * 6 + inside == iota((384, 256), 0)))


def rest_pick(core):
    row = iota((32, 256), 1)
    return ones_where((row % 8 == 6) & (2 * (row // 8) + core == iota((32, 256), 0)))


def sigmoid(v):
    return 1.0 / (1.0 + jnp.exp(-v))


def make_dense_kernel(step):
    def dense_kernel(
        me_ref, rep_ref, a_ref, at_ref, feat_ref, lab_ref, wa_ref, wb_ref, *refs
    ):
        refs = list(refs)
        core = me_ref[2]
        wa = wa_ref[...]
        wb = wb_ref[...]
        w = (mm(top_pick(core), wa) + mm(top_pick(1 - core), wb)).astype(bf16)
        if step:
            rest = mm(rest_pick(core), wa[:, :384]) + mm(rest_pick(1 - core), wb[:, :384])
            rest = rest[:, :128] + rest[:, 128:256] + rest[:, 256:384]
        else:
            rest = refs.pop(0)[...]
        hold_ref, joined_ref, dpre_ref, grad_ref = refs
        out_row = jnp.concatenate([rest[DENSE + k : DENSE + k + 1, :] for k in range(8)], axis=1)
        feats = feat_ref[...]
        bpre = jnp.zeros((SAMPLES, EMB), f32)
        for k in range(DENSE):
            bpre = bpre + feats[:, k : k + 1] * rest[k : k + 1, :]
        bgate = sigmoid(bpre)
        bottom = bpre * bgate
        pooled = mm(a_ref[...], rep_ref[...])
        joined = jnp.concatenate([bottom, pooled[:SAMPLES], pooled[SAMPLES:]], axis=1).astype(bf16)
        pre = mm(joined, w)
        gate = sigmoid(pre)
        hidden = pre * gate
        logit = jnp.sum(hidden * out_row, axis=1, keepdims=True)
        dlogit = sigmoid(logit) - lab_ref[...]
        dpre = (dlogit * out_row * (gate * (1.0 + pre * (1.0 - gate)))).astype(bf16)
        dz = mm_nt(dpre, w)
        both = jnp.concatenate([dz[:, EMB : 2 * EMB], dz[:, 2 * EMB :]], axis=0).astype(bf16)
        hold_ref[...] = mm(at_ref[...], both).astype(bf16)
        joined_ref[...] = joined
        dpre_ref[...] = dpre
        dbottom = dz[:, :EMB] * (bgate * (1.0 + bpre * (1.0 - bgate)))
        for k in range(DENSE):
            grad_ref[k : k + 1, :] = jnp.sum(feats[:, k : k + 1] * dbottom, axis=0, keepdims=True)
        dout = jnp.sum(hidden * dlogit, axis=0, keepdims=True)
        for k in range(8):
            grad_ref[DENSE + k : DENSE + k + 1, :] = dout[:, k * EMB : (k + 1) * EMB]
        grad_ref[DENSE + 8 :, :] = jnp.zeros((32 - DENSE - 8, EMB), f32)

    return dense_kernel


def dense_step(me, rep, a, at, feats, labels, wa, wb, rest, step):
    operands = [me, rep, a, at, feats, labels, wa, wb] + ([] if step else [rest])
    return pl.pallas_call(
        make_dense_kernel(step),
        name="dense_%d" % step,
        in_specs=[sm] + [vm] * (len(operands) - 1),
        out_specs=[vm] * 4,
        out_shape=[
            jax.ShapeDtypeStruct((ALL_SLOTS, EMB), bf16),
            jax.ShapeDtypeStruct((SAMPLES, 384), bf16),
            jax.ShapeDtypeStruct((SAMPLES, HID), bf16),
            jax.ShapeDtypeStruct((32, EMB), f32),
        ],
        compiler_params=params(),
    )(*operands)


def weight_grad_kernel(me_ref, joined_ref, dpre_ref, rest_ref, keep_ref, send_ref):
    core = me_ref[2]
    joined = joined_ref[...]
    dpre = dpre_ref[...]
    rest = rest_ref[...].astype(bf16)
    for which, out in ((core, keep_ref), (1 - core, send_ref)):
        picked = mm(joined, top_pick(which)).astype(bf16)
        out[...] = mm_tn(picked, dpre).astype(out.dtype)
        more = mm_tn(rest_pick(which), rest)
        out[:, :EMB] = (out[:, :EMB].astype(f32) + more).astype(out.dtype)


def weight_grad(me, joined, dpre, rest):
    return pl.pallas_call(
        weight_grad_kernel,
        name="weight_grad",
        in_specs=[sm, vm, vm, vm],
        out_specs=[vm, vm],
        out_shape=[
            jax.ShapeDtypeStruct((256, HID), f32),
            jax.ShapeDtypeStruct((256, HID), bf16),
        ],
        compiler_params=params(),
    )(me, joined, dpre, rest)


def exchange(x, axis="shard", groups=None):
    return lax.all_to_all(x, axis, 0, 0, tiled=True, axis_index_groups=groups)


def other_core(x):
    return lax.ppermute(x, "shard", [(i, i ^ 1) for i in range(NS)])


def to_group(x, d):
    return lax.ppermute(x, "group", [(i, (i + d) % NG) for i in range(NG)])


def from_groups(x):
    return [x] + [to_group(x, d) for d in range(1, NG)]


def spread(block):
    z = exchange(jnp.broadcast_to(block[None], (ZS, 8, HID)), groups=z_groups)
    y = exchange(
        jnp.broadcast_to(z.reshape(1, 64, HID), (YS, 64, HID)), groups=y_groups
    ).reshape(256, HID)
    return y, other_core(y)


def summed(keep, send):
    half = (keep + other_core(send).astype(f32)).astype(bf16).reshape(YS, 64, HID)
    y = exchange(half, groups=y_groups).astype(f32).sum(axis=0)
    z = exchange(y.astype(bf16).reshape(ZS, 8, HID), groups=z_groups)
    return z.astype(f32).sum(axis=0)


def in_three(v):
    a = lax.reduce_precision(v, 8, 7)
    b = lax.reduce_precision(v - a, 8, 7)
    c = v - a - b
    return a, b, c


def body(
    table,
    owners,
    offsets,
    bag_lengths,
    dense_feats,
    labels,
    bottom_weight,
    top_weight,
    out_weight,
    client_group,
):
    shard = lax.axis_index("shard")
    group = lax.axis_index("group")
    me = jnp.stack([shard, group, shard % 2]).astype(i32)
    counts = jnp.sum((client_group[None, :] == jnp.arange(NG)[:, None]).astype(f32), axis=1)
    weights = counts * NG / client_group.shape[0]
    requests, slots = route(me, owners.reshape(4, LOOKS), offsets.reshape(4, LOOKS))
    rest = jnp.concatenate(
        [bottom_weight, out_weight.reshape(8, EMB), jnp.zeros((NS - DENSE - 8, EMB), f32)], 0
    )
    my_rest = lax.dynamic_slice_in_dim(rest, shard, 1, 0)
    received = exchange(requests)
    idx_all = exchange(jnp.broadcast_to(received[None], (NG, NS, 2 * SLOTS)), "group")
    idx_all = idx_all.reshape(NG * NS, 2 * SLOTS)
    wa, wb = spread(jnp.pad(top_weight, ((0, 2), (0, 0))).astype(bf16))
    matrices = [
        pool_matrix(slots[2 * s : 2 * s + 2], bag_lengths[0, s, :, 0]) for s in range(2)
    ]
    table32 = table.astype(f32)
    own_clash = clashes(received)
    clash_all = clashes(idx_all)
    served = gather_first(received, table32)
    total = None
    top_sum = jnp.zeros((8, HID), f32)
    for step in range(2):
        replies = exchange(served.reshape(NS, SLOTS, EMB)).reshape(ALL_SLOTS, EMB)
        hold, joined, dpre, rest_grad = dense_step(
            me,
            replies,
            *matrices[step],
            dense_feats[0, step],
            labels[0, step].astype(f32)[:, None],
            wa,
            wb,
            rest[:32],
            step,
        )
        grads = exchange(hold.reshape(NS, SLOTS, EMB)).reshape(ALL_SLOTS, EMB)
        top_grad = summed(*weight_grad(me, joined, dpre, rest_grad))
        top_sum = top_sum + top_grad
        if step == 0:
            served = owner_step(received, own_clash, grads, table32)
            new = jnp.pad(top_weight, ((0, 2), (0, 0))) - dense_rate * (top_grad / BATCH)
            parts = in_three(my_rest - dense_rate * (top_grad[6:7, :EMB] / BATCH))
            row = jnp.concatenate([*parts, jnp.zeros((1, HID - 3 * EMB), f32)], 1)
            block = jnp.concatenate([new[:6], row, jnp.zeros((1, HID), f32)], 0)
            wa, wb = spread(block.astype(bf16))
        lists = from_groups(grads)
        total = add_lists(me, -emb_rate * weights, idx_all, clash_all, lists, total, step)
    mine = weights[group] * (-dense_rate / BATCH) * top_sum
    a, b, c, d = from_groups(mine)
    dense = (a + c) + (b + d)
    ends = exchange(jnp.broadcast_to(dense[6:7, :EMB][None], (NS, 1, EMB))).reshape(NS, EMB)
    return (
        total,
        dense[:6],
        ends[:DENSE],
        ends[DENSE : DENSE + 8].reshape(HID),
    )


def solution(mesh):
    in_specs = (
        P(None, "shard", None),
        P("group", None, None, "shard", None),
        P("group", None, None, "shard"),
        P("group", None, None, "shard", None),
        P("group", None, "shard", None),
        P("group", None, "shard"),
        P(),
        P("shard", None),
        P(),
        P(),
    )
    out_specs = (P(None, "shard", None), P("shard", None), P(), P())
    return jax.shard_map(body, mesh=mesh, in_specs=in_specs, out_specs=out_specs, check_vma=False)
```

```python
import jax
import jax.numpy as jnp
from jax import lax
from jax.experimental import pallas as pl
from jax.experimental.pallas import tpu as pltpu
from jax.sharding import PartitionSpec as P


emb_rate = 2.0
dense_rate = 0.5
bf16 = jnp.bfloat16
f32 = jnp.float32
i32 = jnp.int32

NS = 64
NG = 4
YS = 4
CAP = 24
SLOTS = 2 * CAP
LOOKS = 512
SAMPLES = 128
EMB = 128
ROWS = 8192
HID = 1024
DENSE = 13
ALL_SLOTS = NS * SLOTS
BATCH = NS * SAMPLES


def params(mb=24):
    return pltpu.CompilerParams(vmem_limit_bytes=mb * 1024 * 1024)


vm = pl.BlockSpec(memory_space=pltpu.VMEM)
sm = pl.BlockSpec(memory_space=pltpu.SMEM)
hb = pl.BlockSpec(memory_space=pl.ANY)


def iota(shape, dim):
    return lax.broadcasted_iota(i32, shape, dim)


def ones_where(mask):
    return jnp.where(mask, 1.0, 0.0).astype(bf16)


def mm(a, b):
    return lax.dot_general(a, b, (((1,), (0,)), ((), ())), preferred_element_type=f32)


def mm_nt(a, b):
    return lax.dot_general(a, b, (((1,), (1,)), ((), ())), preferred_element_type=f32)


def mm_tn(a, b):
    return lax.dot_general(a, b, (((0,), (0,)), ((), ())), preferred_element_type=f32)


def route_kernel(me_ref, own_ref, off_ref, req_ref, slot_ref):
    earlier = ones_where(iota((LOOKS, LOOKS), 0) < iota((LOOKS, LOOKS), 1))
    total = jnp.zeros((NS, 2 * SLOTS), f32)
    count = jnp.zeros((NS, 2 * SLOTS), f32)
    for st in range(4):
        own = own_ref[st : st + 1, :]
        off = off_ref[st : st + 1, :]
        named = iota((NS, LOOKS), 0) == own
        before = mm(ones_where(named), earlier)
        rank = jnp.sum(jnp.where(named, before, 0.0), axis=0, keepdims=True).astype(i32)
        column = ones_where(iota((2 * SLOTS, LOOKS), 0) == rank + st * CAP)
        high = jnp.where(named, (off >> 8).astype(f32), 0.0).astype(bf16)
        low = jnp.where(named, (off & 255).astype(f32), 0.0).astype(bf16)
        total = total + mm_nt(high, column) * 256.0 + mm_nt(low, column)
        count = count + mm_nt(ones_where(named), column)
        slot_ref[st : st + 1, :] = own * SLOTS + (st % 2) * CAP + rank
    spare = me_ref[0] * CAP + iota((NS, 2 * SLOTS), 1) % CAP
    req_ref[...] = jnp.where(count > 0.5, total.astype(i32), spare)


def route(me, own, off):
    return pl.pallas_call(
        route_kernel,
        name="route",
        in_specs=[sm, vm, vm],
        out_specs=[vm, vm],
        out_shape=[
            jax.ShapeDtypeStruct((NS, 2 * SLOTS), i32),
            jax.ShapeDtypeStruct((4, LOOKS), i32),
        ],
        compiler_params=params(),
    )(me, own, off)


def pool_kernel(slot_ref, bag_ref, a_ref, at_ref):
    upto = ones_where(iota((SAMPLES, SAMPLES), 1) <= iota((SAMPLES, SAMPLES), 0))
    below = ones_where(iota((SAMPLES, SAMPLES), 1) < iota((SAMPLES, SAMPLES), 0))
    look = iota((SAMPLES, LOOKS), 1).astype(f32)
    for t in range(2):
        lens = jnp.broadcast_to(bag_ref[t : t + 1, :], (8, SAMPLES)).astype(f32).astype(bf16)
        ends = mm_nt(upto, lens)[:, :1]
        starts = mm_nt(below, lens)[:, :1]
        member = ones_where((look >= starts) & (look < ends))
        slot = slot_ref[t : t + 1, :]
        for q in range(ALL_SLOTS // LOOKS):
            at_slot = ones_where(iota((LOOKS, LOOKS), 0) + q * LOOKS == slot)
            a_ref[t * SAMPLES : (t + 1) * SAMPLES, q * LOOKS : (q + 1) * LOOKS] = mm_nt(
                member, at_slot
            ).astype(bf16)
            at_ref[q * LOOKS : (q + 1) * LOOKS, t * SAMPLES : (t + 1) * SAMPLES] = mm_nt(
                at_slot, member
            ).astype(bf16)


def pool_matrix(slot, bags):
    return pl.pallas_call(
        pool_kernel,
        name="pool_matrix",
        in_specs=[vm, vm],
        out_specs=[vm, vm],
        out_shape=[
            jax.ShapeDtypeStruct((2 * SAMPLES, ALL_SLOTS), bf16),
            jax.ShapeDtypeStruct((ALL_SLOTS, 2 * SAMPLES), bf16),
        ],
        compiler_params=params(),
    )(slot, bags)


def find_clashes(idx):
    lane = iota(idx.shape, 1)
    clash = jnp.zeros(idx.shape, i32)
    for d in range(1, 8):
        same = (idx == jnp.concatenate([idx[:, -d:], idx[:, :-d]], axis=1)) & (lane % 8 >= d)
        clash = clash | jnp.where(same, 1, 0)
    out = jnp.zeros(idx.shape, i32)
    for part in range(4):
        any_of = jnp.max(jnp.where(lane // CAP == part, clash, 0), axis=1, keepdims=True)
        out = jnp.where(lane == part, any_of, out)
    return out


def own_lists_kernel(idx_ref, rows_ref, flags_ref):
    idx = idx_ref[...]
    turned = idx.T
    rows_ref[...] = jnp.concatenate([turned[:SLOTS], turned[SLOTS : 2 * SLOTS]], axis=1)
    flags = find_clashes(idx).T
    flags_ref[...] = jnp.concatenate([flags[0:1] + flags[1:2], flags[2:3] + flags[3:4]], axis=1)


def all_lists_kernel(idx_ref, rows_ref, flags_ref):
    idx = idx_ref[...]
    turned = idx.T
    flags = find_clashes(idx).T
    for part in range(4):
        for half in range(2):
            cut = slice(128 * half, 128 * half + 128)
            rows_ref[part, half] = turned[part * CAP : (part + 1) * CAP, cut]
            flags_ref[part, half : half + 1] = flags[part : part + 1, cut]


def list_rows(idx, kernel, rows, flags):
    return pl.pallas_call(
        kernel,
        in_specs=[vm],
        out_specs=[vm, vm],
        out_shape=[jax.ShapeDtypeStruct(rows, i32), jax.ShapeDtypeStruct(flags, i32)],
        compiler_params=params(),
    )(jnp.pad(idx, ((0, 0), (0, 32))))


def own_lists(idx):
    return list_rows(idx, own_lists_kernel, (SLOTS, 2 * NS), (1, 2 * NS))


def all_lists(idx):
    return list_rows(idx, all_lists_kernel, (4, 2, CAP, 128), (4, 2, 128))


def gather_rows(idx_ref, first, tables, stage):
    def one(s, _):
        base = pl.multiple_of(s * SLOTS, 8)
        for j in range(SLOTS):
            row = idx_ref.at[j][first + s]
            stage[pl.ds(base + j, 1), :] = tables[j // CAP][pl.ds(row, 1), :]
        return 0

    lax.fori_loop(0, NS, one, 0)


def add_rows(lists, clear_of):
    def one(s, _):
        clear = clear_of(s)

        @pl.when(clear)
        def _():
            for b in range(0, CAP, 8):
                held = []
                for numbers, source, rows, start, table in lists:
                    base = start(s)
                    for j in range(b, b + 8):
                        row = numbers(j)[source + s]
                        held.append(
                            (table, row, table[pl.ds(row, 1), :] + rows[pl.ds(base + j, 1), :])
                        )
                for table, row, value in held:
                    table[pl.ds(row, 1), :] = value

        @pl.when(jnp.logical_not(clear))
        def _():
            for numbers, source, rows, start, table in lists:
                base = start(s)
                for j in range(CAP):
                    row = numbers(j)[source + s]
                    table[pl.ds(row, 1), :] = table[pl.ds(row, 1), :] + rows[pl.ds(base + j, 1), :]

        return 0

    lax.fori_loop(0, NS, one, 0)


def gather_kernel(idx_ref, tab_ref, out_ref, tab0, tab1, stage):
    tab0[...] = tab_ref[0].astype(f32)
    tab1[...] = tab_ref[1].astype(f32)
    gather_rows(idx_ref, 0, [tab0, tab1], stage)
    out_ref[...] = stage[...].astype(bf16)


def gather_first(idx, table):
    return pl.pallas_call(
        gather_kernel,
        name="gather_first",
        in_specs=[sm, vm],
        out_specs=vm,
        out_shape=jax.ShapeDtypeStruct((ALL_SLOTS, EMB), bf16),
        scratch_shapes=[
            pltpu.VMEM((ROWS, EMB), f32),
            pltpu.VMEM((ROWS, EMB), f32),
            pltpu.VMEM((ALL_SLOTS, EMB), f32),
        ],
        compiler_params=params(20),
    )(idx, table)


def owner_kernel(idx_ref, clash_ref, grad_ref, tab_ref, out_ref, new0, new1, stage):
    new0[...] = tab_ref[0].astype(f32)
    new1[...] = tab_ref[1].astype(f32)
    stage[...] = grad_ref[...].astype(f32) * -emb_rate
    add_rows(
        [
            (
                lambda j, t=t: idx_ref.at[t * CAP + j],
                0,
                stage,
                lambda s, t=t: pl.multiple_of(s * SLOTS + t * CAP, 8),
                new,
            )
            for t, new in enumerate((new0, new1))
        ],
        lambda s: clash_ref[0, s] == 0,
    )
    gather_rows(idx_ref, NS, [new0, new1], stage)
    out_ref[:, :SLOTS, :] = stage[...].astype(bf16).reshape(NS, SLOTS, EMB)


def owner_step(idx, clash, grads, table):
    return pl.pallas_call(
        owner_kernel,
        name="owner_step",
        in_specs=[sm, sm, vm, vm],
        out_specs=vm,
        out_shape=jax.ShapeDtypeStruct((NS, SLOTS + 32, EMB), bf16),
        scratch_shapes=[
            pltpu.VMEM((ROWS, EMB), f32),
            pltpu.VMEM((ROWS, EMB), f32),
            pltpu.VMEM((ALL_SLOTS, EMB), f32),
        ],
        compiler_params=params(20),
    )(idx, clash, grads, table)


def make_total_kernel(step, t):
    def total_kernel(me_ref, weight_ref, idx_ref, clash_ref, *refs):
        lists = refs[:NG]
        old, out_ref = (refs[NG], refs[NG + 1]) if step or t else (None, refs[NG])
        acc0, acc1, part, stage0, stage1, sems, acc_sem = refs[-7:]
        group = me_ref[1]
        apart = [(group + NG - k) % NG for k in range(NG)]

        def list_copy(d, k):
            rows = lists[d].at[:, pl.ds(0 if step else t * CAP, CAP), :]
            return pltpu.make_async_copy(rows, part.at[k], sems.at[k])

        for k in range(NG):
            for d in range(NG):

                @pl.when(apart[k] == d)
                def _(d=d, k=k):
                    list_copy(d, k).start()

        if step:
            seed = pltpu.make_async_copy(old.at[t], acc0, acc_sem)
            seed.start()
        else:
            acc0[...] = jnp.zeros(acc0.shape, f32)
        acc1[...] = jnp.zeros(acc1.shape, f32)
        for k in range(0, NG, 2):
            for i, stage in enumerate((stage0, stage1)):
                list_copy(0, k + i).wait()
                stage[...] = part[k + i].reshape(NS * CAP, EMB).astype(f32) * weight_ref[k + i]
            if step and k == 0:
                seed.wait()
            halves = [apart[k + i] // 2 for i in range(2)]
            sources = [(apart[k + i] % 2) * NS for i in range(2)]
            add_rows(
                [
                    (
                        lambda j, i=i: idx_ref.at[halves[i], j],
                        sources[i],
                        (stage0, stage1)[i],
                        lambda s: pl.multiple_of(s * CAP, 8),
                        (acc0, acc1)[i],
                    )
                    for i in range(2)
                ],
                lambda s: clash_ref.at[halves[0]][sources[0] + s]
                + clash_ref.at[halves[1]][sources[1] + s]
                == 0,
            )
        acc0[...] = acc0[...] + acc1[...]
        result = pltpu.make_async_copy(acc0, out_ref.at[t], acc_sem)
        result.start()
        result.wait()

    return total_kernel


def add_lists(me, weights, idx, clash, lists, old, step, t):
    part = 2 * step + t
    operands = [me, weights, idx[part], clash[part], *lists] + ([old] if step or t else [])
    return pl.pallas_call(
        make_total_kernel(step, t),
        in_specs=[sm, sm, sm, sm] + [hb] * (len(operands) - 4),
        out_specs=hb,
        out_shape=jax.ShapeDtypeStruct((2, ROWS, EMB), f32),
        input_output_aliases={4 + NG: 0} if step or t else {},
        scratch_shapes=[
            pltpu.VMEM((ROWS, EMB), f32),
            pltpu.VMEM((ROWS, EMB), f32),
            pltpu.VMEM((NG, NS, CAP, EMB), bf16),
            pltpu.VMEM((NS * CAP, EMB), f32),
            pltpu.VMEM((NS * CAP, EMB), f32),
            pltpu.SemaphoreType.DMA((NG,)),
            pltpu.SemaphoreType.DMA,
        ],
        compiler_params=params(16),
    )(*operands)


def block_device(me, other):
    row = iota((384, 256), 1)
    return (2 * (row // 8) + other) ^ me, row % 8


def top_pick(me, other):
    device, inside = block_device(me, other)
    return ones_where((inside < 6) & (device * 6 + inside == iota((384, 256), 0)))


def rest_pick(me, other):
    device, inside = block_device(me, other)
    return ones_where((inside == 6) & (device == iota((384, 256), 0)))[:32]


def piece_picks(b):
    row = iota((384, NS * 16), 1)
    want = iota((384, NS * 16), 0)
    inside = row % 16 - 8 * b
    top = (inside >= 0) & (inside < 6) & ((row // 16) * 6 + inside == want)
    rest = (inside == 6) & (row // 16 == want)
    return ones_where(top), ones_where(rest)[:32]


def sigmoid(v):
    return 1.0 / (1.0 + jnp.exp(-v))


def make_dense_kernel(step):
    def dense_kernel(
        me_ref, a_ref, at_ref, feat_ref, lab_ref, wa_ref, wb_ref, *refs
    ):
        refs = list(refs)
        me = me_ref[0]
        if step:
            core = me % 2
            halves = []
            rests = []
            for part in (wa_ref[:, SLOTS:, :], wb_ref[...]):
                tiles = [part[:, 16 * u : 16 * u + 16, :].reshape(NS * 16, EMB) for u in range(2)]
                picks = [piece_picks(b) for b in range(2)]
                halves.append(
                    jnp.concatenate([mm(picks[j % 2][0], tiles[j // 2]) for j in range(4)], axis=1)
                )
                rests.append(sum(mm(picks[j % 2][1], tiles[j // 2]) for j in range(3)))
            w = jnp.concatenate(
                [
                    jnp.where(core == 0, halves[0], halves[1]),
                    jnp.where(core == 0, halves[1], halves[0]),
                ],
                axis=1,
            ).astype(bf16)
            rest = jnp.where(core == 0, rests[0], rests[1])
            rep = wa_ref[:, :SLOTS, :].reshape(ALL_SLOTS, EMB)
        else:
            w = (mm(top_pick(me, 0), wa_ref[...]) + mm(top_pick(me, 1), wb_ref[...])).astype(bf16)
            rest = refs.pop(0)[...]
            rep = refs.pop(0)[...]
        hold_ref, joined_ref, dpre_ref, grad_ref = refs
        out_row = jnp.concatenate([rest[DENSE + k : DENSE + k + 1, :] for k in range(8)], axis=1)
        feats = feat_ref[...]
        bpre = jnp.zeros((SAMPLES, EMB), f32)
        for k in range(DENSE):
            bpre = bpre + feats[:, k : k + 1] * rest[k : k + 1, :]
        bgate = sigmoid(bpre)
        bottom = bpre * bgate
        pooled = mm(a_ref[...], rep)
        joined = jnp.concatenate([bottom, pooled[:SAMPLES], pooled[SAMPLES:]], axis=1).astype(bf16)
        pre = mm(joined, w)
        gate = sigmoid(pre)
        hidden = pre * gate
        logit = jnp.sum(hidden * out_row, axis=1, keepdims=True)
        dlogit = sigmoid(logit) - lab_ref[...]
        dpre = (dlogit * out_row * (gate * (1.0 + pre * (1.0 - gate)))).astype(bf16)
        dz = mm_nt(dpre, w)
        both = jnp.concatenate([dz[:, EMB : 2 * EMB], dz[:, 2 * EMB :]], axis=0).astype(bf16)
        hold_ref[...] = mm(at_ref[...], both).astype(bf16)
        joined_ref[...] = joined
        dpre_ref[...] = dpre
        dbottom = dz[:, :EMB] * (bgate * (1.0 + bpre * (1.0 - bgate)))
        for k in range(DENSE):
            grad_ref[k : k + 1, :] = jnp.sum(feats[:, k : k + 1] * dbottom, axis=0, keepdims=True)
        dout = jnp.sum(hidden * dlogit, axis=0, keepdims=True)
        for k in range(8):
            grad_ref[DENSE + k : DENSE + k + 1, :] = dout[:, k * EMB : (k + 1) * EMB]
        grad_ref[DENSE + 8 :, :] = jnp.zeros((32 - DENSE - 8, EMB), f32)

    return dense_kernel


def dense_step(me, a, at, feats, labels, more, step):
    operands = [me, a, at, feats, labels, *more]
    return pl.pallas_call(
        make_dense_kernel(step),
        in_specs=[sm] + [vm] * (len(operands) - 1),
        out_specs=[vm] * 4,
        out_shape=[
            jax.ShapeDtypeStruct((ALL_SLOTS, EMB), bf16),
            jax.ShapeDtypeStruct((SAMPLES, 384), bf16),
            jax.ShapeDtypeStruct((SAMPLES, HID), bf16),
            jax.ShapeDtypeStruct((32, EMB), f32),
        ],
        compiler_params=params(),
    )(*operands)


def weight_grad_kernel(me_ref, joined_ref, dpre_ref, rest_ref, keep_ref, send_ref):
    me = me_ref[0]
    joined = joined_ref[...]
    dpre = dpre_ref[...]
    rest = rest_ref[...].astype(bf16)
    for which, out in ((0, keep_ref), (1, send_ref)):
        picked = mm(joined, top_pick(me, which)).astype(bf16)
        out[...] = mm_tn(picked, dpre).astype(out.dtype)
        more = mm_tn(rest_pick(me, which), rest)
        out[:, :EMB] = (out[:, :EMB].astype(f32) + more).astype(out.dtype)


def weight_grad(me, joined, dpre, rest):
    return pl.pallas_call(
        weight_grad_kernel,
        name="weight_grad",
        in_specs=[sm, vm, vm, vm],
        out_specs=[vm, vm],
        out_shape=[
            jax.ShapeDtypeStruct((256, HID), f32),
            jax.ShapeDtypeStruct((256, HID), bf16),
        ],
        compiler_params=params(),
    )(me, joined, dpre, rest)


def exchange(x):
    return lax.all_to_all(x, "shard", 0, 0, tiled=True)


def to_group(x, d):
    return lax.ppermute(x, "group", [(i, (i + d) % NG) for i in range(NG)])


def from_groups(x):
    return [x] + [to_group(x, d) for d in range(1, NG)]


def swap(x, bits):
    return lax.ppermute(x, "shard", [(i, i ^ bits) for i in range(NS)])


def spread(block):
    have = block
    for bits in (2, 4, 8):
        have = jnp.concatenate([have, swap(have, bits)], 0)
    have = jnp.concatenate([have] + [swap(have, 16 * d) for d in range(1, YS)], 0)
    return have, swap(have, 1)


def summed(keep, send):
    half = keep + swap(send, 1).astype(f32)
    low = half[64:].astype(bf16)
    got = [swap(low[64 * d - 64 : 64 * d], 16 * d).astype(f32) for d in range(1, YS)]
    half = half[:64] + got[0] + got[1] + got[2]
    half = half[:32] + swap(half[32:].astype(bf16), 8).astype(f32)
    got = [swap(half[8 * d : 8 * d + 8], 2 * d) for d in range(1, 4)]
    return half[:8] + got[0] + got[1] + got[2]


def in_three(v):
    a = lax.reduce_precision(v, 8, 7)
    b = lax.reduce_precision(v - a, 8, 7)
    c = v - a - b
    return a, b, c


def whole_round(
    table,
    owners,
    offsets,
    bag_lengths,
    dense_feats,
    labels,
    bottom_weight,
    top_weight,
    out_weight,
    client_group,
):
    shard = lax.axis_index("shard")
    group = lax.axis_index("group")
    me = jnp.stack([shard, group]).astype(i32)
    counts = jnp.sum((client_group[None, :] == jnp.arange(NG)[:, None]).astype(f32), axis=1)
    weights = counts * NG / client_group.shape[0]
    requests, slots = route(me, owners.reshape(4, LOOKS), offsets.reshape(4, LOOKS))
    rest = jnp.concatenate(
        [bottom_weight, out_weight.reshape(8, EMB), jnp.zeros((NS - DENSE - 8, EMB), f32)], 0
    )
    my_rest = lax.dynamic_slice_in_dim(rest, shard, 1, 0)
    received = exchange(requests)
    idx_all = jnp.concatenate(from_groups(received), 0)
    first_blocks = spread(jnp.pad(top_weight, ((0, 2), (0, 0))).astype(bf16))
    matrices = []
    for s in range(2):
        matrices.append(pool_matrix(slots[2 * s : 2 * s + 2], bag_lengths[0, s, :, 0]))
    own_idx, own_clash = own_lists(received)
    all_idx, all_clash = all_lists(idx_all)
    served = gather_first(own_idx, table).reshape(NS, SLOTS, EMB)
    total = None
    top_sum = jnp.zeros((8, HID), f32)
    for step in range(2):
        replies = exchange(served)
        if step:
            more = [replies, swap(replies[:, SLOTS:], 1)]
        else:
            more = [*first_blocks, rest[:32], replies.reshape(ALL_SLOTS, EMB)]
        hold, joined, dpre, rest_grad = dense_step(
            me,
            *matrices[step],
            dense_feats[0, step],
            labels[0, step].astype(f32)[:, None],
            more,
            step,
        )
        grads = exchange(hold.reshape(NS, SLOTS, EMB))
        parts = weight_grad(me, joined, dpre, rest_grad)
        top_grad = summed(*parts)
        top_sum = top_sum + top_grad
        if step == 0:
            served = owner_step(own_idx, own_clash, grads.reshape(ALL_SLOTS, EMB), table)
            new = jnp.pad(top_weight, ((0, 2), (0, 0))) - dense_rate * (top_grad / BATCH)
            parts = in_three(my_rest - dense_rate * (top_grad[6:7, :EMB] / BATCH))
            row = jnp.concatenate([*parts, jnp.zeros((1, HID - 3 * EMB), f32)], 1)
            block = jnp.concatenate([new[:6], row, jnp.zeros((1, HID), f32)], 0).astype(bf16)
            tiles = jnp.concatenate([block[:, EMB * j : EMB * (j + 1)] for j in range(8)], 0)
            tiles = jnp.broadcast_to(tiles.reshape(1, 2, 32, EMB), (NS // 2, 2, 32, EMB))
            served = served.at[:, SLOTS:, :].set(tiles.reshape(NS, 32, EMB))
            lists = from_groups(grads)
            for t in range(2):
                total = add_lists(me, -emb_rate * weights, all_idx, all_clash, lists, total, 0, t)
        else:
            for t in range(2):
                lists = from_groups(grads[:, t * CAP : (t + 1) * CAP])
                total = add_lists(me, -emb_rate * weights, all_idx, all_clash, lists, total, 1, t)
    mine = weights[group] * (-dense_rate / BATCH) * top_sum
    a, b, c, d = from_groups(mine)
    dense = (a + c) + (b + d)
    ends = exchange(jnp.broadcast_to(dense[6:7, :EMB][None], (NS, 1, EMB))).reshape(NS, EMB)
    return (
        total,
        dense[:6],
        ends[:DENSE],
        ends[DENSE : DENSE + 8].reshape(HID),
    )


def solution(mesh):
    in_specs = (
        P(None, "shard", None),
        P("group", None, None, "shard", None),
        P("group", None, None, "shard"),
        P("group", None, None, "shard", None),
        P("group", None, "shard", None),
        P("group", None, "shard"),
        P(),
        P("shard", None),
        P(),
        P(),
    )
    out_specs = (P(None, "shard", None), P("shard", None), P(), P())
    return jax.shard_map(whole_round, mesh=mesh, in_specs=in_specs, out_specs=out_specs, check_vma=False)
```

```python
import jax
import jax.numpy as jnp
from jax import lax
from jax.experimental import pallas as pl
from jax.experimental.pallas import tpu as pltpu
from jax.sharding import PartitionSpec as P


emb_rate = 2.0
dense_rate = 0.5
bf16 = jnp.bfloat16
f32 = jnp.float32
i32 = jnp.int32

NS = 64
NG = 4
YS = 4
CAP = 24
SLOTS = 2 * CAP
LOOKS = 512
SAMPLES = 128
EMB = 128
ROWS = 8192
HID = 1024
DENSE = 13
ALL_SLOTS = NS * SLOTS
BATCH = NS * SAMPLES


def params(mb=24):
    return pltpu.CompilerParams(vmem_limit_bytes=mb * 1024 * 1024)


vm = pl.BlockSpec(memory_space=pltpu.VMEM)
sm = pl.BlockSpec(memory_space=pltpu.SMEM)
hb = pl.BlockSpec(memory_space=pl.ANY)


def iota(shape, dim):
    return lax.broadcasted_iota(i32, shape, dim)


def ones_where(mask):
    return jnp.where(mask, 1.0, 0.0).astype(bf16)


def mm(a, b):
    return lax.dot_general(a, b, (((1,), (0,)), ((), ())), preferred_element_type=f32)


def mm_nt(a, b):
    return lax.dot_general(a, b, (((1,), (1,)), ((), ())), preferred_element_type=f32)


def mm_tn(a, b):
    return lax.dot_general(a, b, (((0,), (0,)), ((), ())), preferred_element_type=f32)


def route_kernel(me_ref, own_ref, off_ref, req_ref, slot_ref):
    earlier = ones_where(iota((LOOKS, LOOKS), 0) < iota((LOOKS, LOOKS), 1))
    total = jnp.zeros((NS, 2 * SLOTS), f32)
    count = jnp.zeros((NS, 2 * SLOTS), f32)
    for st in range(4):
        own = own_ref[st : st + 1, :]
        off = off_ref[st : st + 1, :]
        named = iota((NS, LOOKS), 0) == own
        before = mm(ones_where(named), earlier)
        rank = jnp.sum(jnp.where(named, before, 0.0), axis=0, keepdims=True).astype(i32)
        column = ones_where(iota((2 * SLOTS, LOOKS), 0) == rank + st * CAP)
        high = jnp.where(named, (off >> 8).astype(f32), 0.0).astype(bf16)
        low = jnp.where(named, (off & 255).astype(f32), 0.0).astype(bf16)
        total = total + mm_nt(high, column) * 256.0 + mm_nt(low, column)
        count = count + mm_nt(ones_where(named), column)
        slot_ref[st : st + 1, :] = own * SLOTS + (st % 2) * CAP + rank
    spare = me_ref[0] * CAP + iota((NS, 2 * SLOTS), 1) % CAP
    req_ref[...] = jnp.where(count > 0.5, total.astype(i32), spare)


def route(me, own, off):
    return pl.pallas_call(
        route_kernel,
        name="route",
        in_specs=[sm, vm, vm],
        out_specs=[vm, vm],
        out_shape=[
            jax.ShapeDtypeStruct((NS, 2 * SLOTS), i32),
            jax.ShapeDtypeStruct((4, LOOKS), i32),
        ],
        compiler_params=params(),
    )(me, own, off)


def pool_kernel(slot_ref, bag_ref, a_ref, at_ref):
    upto = ones_where(iota((SAMPLES, SAMPLES), 1) <= iota((SAMPLES, SAMPLES), 0))
    below = ones_where(iota((SAMPLES, SAMPLES), 1) < iota((SAMPLES, SAMPLES), 0))
    look = iota((SAMPLES, LOOKS), 1).astype(f32)
    for t in range(2):
        lens = jnp.broadcast_to(bag_ref[t : t + 1, :], (8, SAMPLES)).astype(f32).astype(bf16)
        ends = mm_nt(upto, lens)[:, :1]
        starts = mm_nt(below, lens)[:, :1]
        member = ones_where((look >= starts) & (look < ends))
        slot = slot_ref[t : t + 1, :]
        for q in range(ALL_SLOTS // LOOKS):
            at_slot = ones_where(iota((LOOKS, LOOKS), 0) + q * LOOKS == slot)
            a_ref[t * SAMPLES : (t + 1) * SAMPLES, q * LOOKS : (q + 1) * LOOKS] = mm_nt(
                member, at_slot
            ).astype(bf16)
            at_ref[q * LOOKS : (q + 1) * LOOKS, t * SAMPLES : (t + 1) * SAMPLES] = mm_nt(
                at_slot, member
            ).astype(bf16)


def pool_matrix(slot, bags):
    return pl.pallas_call(
        pool_kernel,
        name="pool_matrix",
        in_specs=[vm, vm],
        out_specs=[vm, vm],
        out_shape=[
            jax.ShapeDtypeStruct((2 * SAMPLES, ALL_SLOTS), bf16),
            jax.ShapeDtypeStruct((ALL_SLOTS, 2 * SAMPLES), bf16),
        ],
        compiler_params=params(),
    )(slot, bags)


def find_clashes(idx):
    lane = iota(idx.shape, 1)
    clash = jnp.zeros(idx.shape, i32)
    for d in range(1, 8):
        same = (idx == jnp.concatenate([idx[:, -d:], idx[:, :-d]], axis=1)) & (lane % 8 >= d)
        clash = clash | jnp.where(same, 1, 0)
    out = jnp.zeros(idx.shape, i32)
    for part in range(4):
        any_of = jnp.max(jnp.where(lane // CAP == part, clash, 0), axis=1, keepdims=True)
        out = jnp.where(lane == part, any_of, out)
    return out


def own_lists_kernel(idx_ref, rows_ref, flags_ref):
    idx = idx_ref[...]
    turned = idx.T
    rows_ref[...] = jnp.concatenate([turned[:SLOTS], turned[SLOTS : 2 * SLOTS]], axis=1)
    flags = find_clashes(idx).T
    flags_ref[...] = jnp.concatenate([flags[0:1] + flags[1:2], flags[2:3] + flags[3:4]], axis=1)


def all_lists_kernel(idx_ref, rows_ref, flags_ref):
    idx = idx_ref[...]
    turned = idx.T
    flags = find_clashes(idx).T
    for part in range(4):
        for half in range(2):
            cut = slice(128 * half, 128 * half + 128)
            rows_ref[part, half] = turned[part * CAP : (part + 1) * CAP, cut]
            flags_ref[part, half : half + 1] = flags[part : part + 1, cut]


def list_rows(idx, kernel, rows, flags):
    return pl.pallas_call(
        kernel,
        in_specs=[vm],
        out_specs=[vm, vm],
        out_shape=[jax.ShapeDtypeStruct(rows, i32), jax.ShapeDtypeStruct(flags, i32)],
        compiler_params=params(),
    )(jnp.pad(idx, ((0, 0), (0, 32))))


def own_lists(idx):
    return list_rows(idx, own_lists_kernel, (SLOTS, 2 * NS), (1, 2 * NS))


def all_lists(idx):
    return list_rows(idx, all_lists_kernel, (4, 2, CAP, 128), (4, 2, 128))


def gather_rows(idx_ref, first, tables, stage):
    def one(s, _):
        base = pl.multiple_of(s * SLOTS, 8)
        for j in range(SLOTS):
            row = idx_ref.at[j][first + s]
            stage[pl.ds(base + j, 1), :] = tables[j // CAP][pl.ds(row, 1), :]
        return 0

    lax.fori_loop(0, NS, one, 0)


def add_rows(lists, clear_of):
    def one(s, _):
        clear = clear_of(s)

        @pl.when(clear)
        def _():
            for b in range(0, CAP, 8):
                held = []
                for numbers, source, rows, start, table in lists:
                    base = start(s)
                    for j in range(b, b + 8):
                        row = numbers(j)[source + s]
                        held.append(
                            (table, row, table[pl.ds(row, 1), :] + rows[pl.ds(base + j, 1), :])
                        )
                for table, row, value in held:
                    table[pl.ds(row, 1), :] = value

        @pl.when(jnp.logical_not(clear))
        def _():
            for numbers, source, rows, start, table in lists:
                base = start(s)
                for j in range(CAP):
                    row = numbers(j)[source + s]
                    table[pl.ds(row, 1), :] = table[pl.ds(row, 1), :] + rows[pl.ds(base + j, 1), :]

        return 0

    lax.fori_loop(0, NS, one, 0)


def gather_kernel(idx_ref, tab_ref, out_ref, tab0, tab1, stage):
    tab0[...] = tab_ref[0].astype(f32)
    tab1[...] = tab_ref[1].astype(f32)
    gather_rows(idx_ref, 0, [tab0, tab1], stage)
    out_ref[...] = stage[...].astype(bf16)


def gather_first(idx, table):
    return pl.pallas_call(
        gather_kernel,
        name="gather_first",
        in_specs=[sm, vm],
        out_specs=vm,
        out_shape=jax.ShapeDtypeStruct((ALL_SLOTS, EMB), bf16),
        scratch_shapes=[
            pltpu.VMEM((ROWS, EMB), f32),
            pltpu.VMEM((ROWS, EMB), f32),
            pltpu.VMEM((ALL_SLOTS, EMB), f32),
        ],
        compiler_params=params(20),
    )(idx, table)


def owner_kernel(idx_ref, clash_ref, grad_ref, tab_ref, out_ref, new0, new1, stage):
    new0[...] = tab_ref[0].astype(f32)
    new1[...] = tab_ref[1].astype(f32)
    stage[...] = grad_ref[...].astype(f32) * -emb_rate
    add_rows(
        [
            (
                lambda j, t=t: idx_ref.at[t * CAP + j],
                0,
                stage,
                lambda s, t=t: pl.multiple_of(s * SLOTS + t * CAP, 8),
                new,
            )
            for t, new in enumerate((new0, new1))
        ],
        lambda s: clash_ref[0, s] == 0,
    )
    gather_rows(idx_ref, NS, [new0, new1], stage)
    out_ref[:, :SLOTS, :] = stage[...].astype(bf16).reshape(NS, SLOTS, EMB)


def owner_step(idx, clash, grads, table):
    return pl.pallas_call(
        owner_kernel,
        name="owner_step",
        in_specs=[sm, sm, vm, vm],
        out_specs=vm,
        out_shape=jax.ShapeDtypeStruct((NS, SLOTS + 32, EMB), bf16),
        scratch_shapes=[
            pltpu.VMEM((ROWS, EMB), f32),
            pltpu.VMEM((ROWS, EMB), f32),
            pltpu.VMEM((ALL_SLOTS, EMB), f32),
        ],
        compiler_params=params(20),
    )(idx, clash, grads, table)


def make_total_kernel(step, t):
    def total_kernel(me_ref, weight_ref, idx_ref, clash_ref, *refs):
        lists = refs[:NG]
        old, out_ref = (refs[NG], refs[NG + 1]) if step or t else (None, refs[NG])
        acc0, acc1, part, stage0, stage1, sems, acc_sem, out_sems = refs[-8:]
        group = me_ref[1]

        def list_copy(d, k):
            rows = lists[d].at[:, pl.ds(0 if step else t * CAP, CAP), :]
            return pltpu.make_async_copy(rows, part.at[k], sems.at[k])

        def apart(k):
            return (group + NG - k) % NG

        def fetch(k, _):
            for d in range(NG):

                @pl.when(apart(k) == d)
                def _(d=d):
                    list_copy(d, k).start()

            return 0

        lax.fori_loop(0, NG, fetch, 0)
        if step:
            seed = pltpu.make_async_copy(old.at[t], acc0, acc_sem)
            seed.start()

        def clear(c, _):
            rows = pl.ds(pl.multiple_of(c * 512, 512), 512)
            zero = jnp.zeros((512, EMB), f32)
            if not step:
                acc0[rows, :] = zero
            acc1[rows, :] = zero
            return 0

        lax.fori_loop(0, ROWS // 512, clear, 0)
        if step:
            seed.wait()

        def pair(p, _):
            ks = [2 * p, 2 * p + 1]
            for k, stage in zip(ks, (stage0, stage1)):
                list_copy(0, k).wait()

                def widen(c, _):
                    rows = part[k, pl.ds(c * 16, 16)].reshape(16 * CAP, EMB)
                    at = pl.multiple_of(c * 16 * CAP, 16 * CAP)
                    stage[pl.ds(at, 16 * CAP), :] = rows.astype(f32) * weight_ref[k]
                    return 0

                lax.fori_loop(0, NS // 16, widen, 0)
            halves = [apart(k) // 2 for k in ks]
            sources = [(apart(k) % 2) * NS for k in ks]
            add_rows(
                [
                    (
                        lambda j, i=i: idx_ref.at[halves[i], j],
                        sources[i],
                        (stage0, stage1)[i],
                        lambda s: pl.multiple_of(s * CAP, 8),
                        (acc0, acc1)[i],
                    )
                    for i in range(2)
                ],
                lambda s: clash_ref.at[halves[0]][sources[0] + s]
                + clash_ref.at[halves[1]][sources[1] + s]
                == 0,
            )
            return 0

        lax.fori_loop(0, NG // 2, pair, 0)

        def result(c):
            rows = pl.ds(pl.multiple_of(c * 1024, 1024), 1024)
            return pltpu.make_async_copy(acc0.at[rows], out_ref.at[t, rows], out_sems.at[c])

        def finish(c, _):
            for half in range(2):
                rows = pl.ds(pl.multiple_of(c * 1024 + half * 512, 512), 512)
                acc0[rows, :] = acc0[rows, :] + acc1[rows, :]
            result(c).start()
            return 0

        def drain(c, _):
            result(c).wait()
            return 0

        lax.fori_loop(0, ROWS // 1024, finish, 0)
        lax.fori_loop(0, ROWS // 1024, drain, 0)

    return total_kernel


def add_lists(me, weights, idx, clash, lists, old, step, t):
    part = 2 * step + t
    operands = [me, weights, idx[part], clash[part], *lists] + ([old] if step or t else [])
    return pl.pallas_call(
        make_total_kernel(step, t),
        in_specs=[sm, sm, sm, sm] + [hb] * (len(operands) - 4),
        out_specs=hb,
        out_shape=jax.ShapeDtypeStruct((2, ROWS, EMB), f32),
        input_output_aliases={4 + NG: 0} if step or t else {},
        scratch_shapes=[
            pltpu.VMEM((ROWS, EMB), f32),
            pltpu.VMEM((ROWS, EMB), f32),
            pltpu.VMEM((NG, NS, CAP, EMB), bf16),
            pltpu.VMEM((NS * CAP, EMB), f32),
            pltpu.VMEM((NS * CAP, EMB), f32),
            pltpu.SemaphoreType.DMA((NG,)),
            pltpu.SemaphoreType.DMA,
            pltpu.SemaphoreType.DMA((ROWS // 1024,)),
        ],
        compiler_params=params(16),
    )(*operands)


def block_device(me, other):
    row = iota((384, 256), 1)
    return (2 * (row // 8) + other) ^ me, row % 8


def top_pick(me, other):
    device, inside = block_device(me, other)
    return ones_where((inside < 6) & (device * 6 + inside == iota((384, 256), 0)))


def rest_pick(me, other):
    device, inside = block_device(me, other)
    return ones_where((inside == 6) & (device == iota((384, 256), 0)))[:32]


def piece_picks(b):
    row = iota((384, NS * 16), 1)
    want = iota((384, NS * 16), 0)
    inside = row % 16 - 8 * b
    top = (inside >= 0) & (inside < 6) & ((row // 16) * 6 + inside == want)
    rest = (inside == 6) & (row // 16 == want)
    return ones_where(top), ones_where(rest)[:32]


def sigmoid(v):
    return 1.0 / (1.0 + jnp.exp(-v))


def make_dense_kernel(step):
    def dense_kernel(
        me_ref, a_ref, at_ref, feat_ref, lab_ref, wa_ref, wb_ref, *refs
    ):
        refs = list(refs)
        me = me_ref[0]
        if step:
            core = me % 2
            halves = []
            rests = []
            for part in (wa_ref[:, SLOTS:, :], wb_ref[...]):
                tiles = [part[:, 16 * u : 16 * u + 16, :].reshape(NS * 16, EMB) for u in range(2)]
                picks = [piece_picks(b) for b in range(2)]
                halves.append(
                    jnp.concatenate([mm(picks[j % 2][0], tiles[j // 2]) for j in range(4)], axis=1)
                )
                rests.append(sum(mm(picks[j % 2][1], tiles[j // 2]) for j in range(3)))
            w = jnp.concatenate(
                [
                    jnp.where(core == 0, halves[0], halves[1]),
                    jnp.where(core == 0, halves[1], halves[0]),
                ],
                axis=1,
            ).astype(bf16)
            rest = jnp.where(core == 0, rests[0], rests[1])
            rep = wa_ref[:, :SLOTS, :].reshape(ALL_SLOTS, EMB)
        else:
            w = (mm(top_pick(me, 0), wa_ref[...]) + mm(top_pick(me, 1), wb_ref[...])).astype(bf16)
            rest = refs.pop(0)[...]
            rep = refs.pop(0)[...]
        hold_ref, joined_ref, dpre_ref, grad_ref = refs
        out_row = jnp.concatenate([rest[DENSE + k : DENSE + k + 1, :] for k in range(8)], axis=1)
        feats = feat_ref[...]
        bpre = jnp.zeros((SAMPLES, EMB), f32)
        for k in range(DENSE):
            bpre = bpre + feats[:, k : k + 1] * rest[k : k + 1, :]
        bgate = sigmoid(bpre)
        bottom = bpre * bgate
        pooled = mm(a_ref[...], rep)
        joined = jnp.concatenate([bottom, pooled[:SAMPLES], pooled[SAMPLES:]], axis=1).astype(bf16)
        pre = mm(joined, w)
        gate = sigmoid(pre)
        hidden = pre * gate
        logit = jnp.sum(hidden * out_row, axis=1, keepdims=True)
        dlogit = sigmoid(logit) - lab_ref[...]
        dpre = (dlogit * out_row * (gate * (1.0 + pre * (1.0 - gate)))).astype(bf16)
        dz = mm_nt(dpre, w)
        both = jnp.concatenate([dz[:, EMB : 2 * EMB], dz[:, 2 * EMB :]], axis=0).astype(bf16)
        hold_ref[...] = mm(at_ref[...], both).astype(bf16)
        joined_ref[...] = joined
        dpre_ref[...] = dpre
        dbottom = dz[:, :EMB] * (bgate * (1.0 + bpre * (1.0 - bgate)))
        for k in range(DENSE):
            grad_ref[k : k + 1, :] = jnp.sum(feats[:, k : k + 1] * dbottom, axis=0, keepdims=True)
        dout = jnp.sum(hidden * dlogit, axis=0, keepdims=True)
        for k in range(8):
            grad_ref[DENSE + k : DENSE + k + 1, :] = dout[:, k * EMB : (k + 1) * EMB]
        grad_ref[DENSE + 8 :, :] = jnp.zeros((32 - DENSE - 8, EMB), f32)

    return dense_kernel


def dense_step(me, a, at, feats, labels, more, step):
    operands = [me, a, at, feats, labels, *more]
    return pl.pallas_call(
        make_dense_kernel(step),
        in_specs=[sm] + [vm] * (len(operands) - 1),
        out_specs=[vm] * 4,
        out_shape=[
            jax.ShapeDtypeStruct((ALL_SLOTS, EMB), bf16),
            jax.ShapeDtypeStruct((SAMPLES, 384), bf16),
            jax.ShapeDtypeStruct((SAMPLES, HID), bf16),
            jax.ShapeDtypeStruct((32, EMB), f32),
        ],
        compiler_params=params(),
    )(*operands)


def weight_grad_kernel(me_ref, joined_ref, dpre_ref, rest_ref, keep_ref, send_ref):
    me = me_ref[0]
    joined = joined_ref[...]
    dpre = dpre_ref[...]
    rest = rest_ref[...].astype(bf16)
    for which, out in ((0, keep_ref), (1, send_ref)):
        picked = mm(joined, top_pick(me, which)).astype(bf16)
        out[...] = mm_tn(picked, dpre).astype(out.dtype)
        more = mm_tn(rest_pick(me, which), rest)
        out[:, :EMB] = (out[:, :EMB].astype(f32) + more).astype(out.dtype)


def weight_grad(me, joined, dpre, rest):
    return pl.pallas_call(
        weight_grad_kernel,
        name="weight_grad",
        in_specs=[sm, vm, vm, vm],
        out_specs=[vm, vm],
        out_shape=[
            jax.ShapeDtypeStruct((256, HID), f32),
            jax.ShapeDtypeStruct((256, HID), bf16),
        ],
        compiler_params=params(),
    )(me, joined, dpre, rest)


def exchange(x):
    return lax.all_to_all(x, "shard", 0, 0, tiled=True)


def to_group(x, d):
    return lax.ppermute(x, "group", [(i, (i + d) % NG) for i in range(NG)])


def from_groups(x):
    return [x] + [to_group(x, d) for d in range(1, NG)]


def swap(x, bits):
    return lax.ppermute(x, "shard", [(i, i ^ bits) for i in range(NS)])


def spread(block):
    have = block
    for bits in (2, 4, 8):
        have = jnp.concatenate([have, swap(have, bits)], 0)
    have = jnp.concatenate([have] + [swap(have, 16 * d) for d in range(1, YS)], 0)
    return have, swap(have, 1)


def summed(keep, send):
    half = keep + swap(send, 1).astype(f32)
    low = half[64:].astype(bf16)
    got = [swap(low[64 * d - 64 : 64 * d], 16 * d).astype(f32) for d in range(1, YS)]
    half = half[:64] + got[0] + got[1] + got[2]
    half = half[:32] + swap(half[32:].astype(bf16), 8).astype(f32)
    got = [swap(half[8 * d : 8 * d + 8], 2 * d) for d in range(1, 4)]
    return half[:8] + got[0] + got[1] + got[2]


def in_three(v):
    a = lax.reduce_precision(v, 8, 7)
    b = lax.reduce_precision(v - a, 8, 7)
    c = v - a - b
    return a, b, c


def whole_round(
    table,
    owners,
    offsets,
    bag_lengths,
    dense_feats,
    labels,
    bottom_weight,
    top_weight,
    out_weight,
    client_group,
):
    shard = lax.axis_index("shard")
    group = lax.axis_index("group")
    me = jnp.stack([shard, group]).astype(i32)
    counts = jnp.sum((client_group[None, :] == jnp.arange(NG)[:, None]).astype(f32), axis=1)
    weights = counts * NG / client_group.shape[0]
    requests, slots = route(me, owners.reshape(4, LOOKS), offsets.reshape(4, LOOKS))
    rest = jnp.concatenate(
        [bottom_weight, out_weight.reshape(8, EMB), jnp.zeros((NS - DENSE - 8, EMB), f32)], 0
    )
    my_rest = lax.dynamic_slice_in_dim(rest, shard, 1, 0)
    received = exchange(requests)
    idx_all = jnp.concatenate(from_groups(received), 0)
    first_blocks = spread(jnp.pad(top_weight, ((0, 2), (0, 0))).astype(bf16))
    matrices = []
    for s in range(2):
        matrices.append(pool_matrix(slots[2 * s : 2 * s + 2], bag_lengths[0, s, :, 0]))
    own_idx, own_clash = own_lists(received)
    all_idx, all_clash = all_lists(idx_all)
    served = gather_first(own_idx, table).reshape(NS, SLOTS, EMB)
    total = None
    top_sum = jnp.zeros((8, HID), f32)
    for step in range(2):
        replies = exchange(served)
        if step:
            more = [replies, swap(replies[:, SLOTS:], 1)]
        else:
            more = [*first_blocks, rest[:32], replies.reshape(ALL_SLOTS, EMB)]
        hold, joined, dpre, rest_grad = dense_step(
            me,
            *matrices[step],
            dense_feats[0, step],
            labels[0, step].astype(f32)[:, None],
            more,
            step,
        )
        grads = exchange(hold.reshape(NS, SLOTS, EMB))
        parts = weight_grad(me, joined, dpre, rest_grad)
        top_grad = summed(*parts)
        top_sum = top_sum + top_grad
        if step == 0:
            served = owner_step(own_idx, own_clash, grads.reshape(ALL_SLOTS, EMB), table)
            new = jnp.pad(top_weight, ((0, 2), (0, 0))) - dense_rate * (top_grad / BATCH)
            parts = in_three(my_rest - dense_rate * (top_grad[6:7, :EMB] / BATCH))
            row = jnp.concatenate([*parts, jnp.zeros((1, HID - 3 * EMB), f32)], 1)
            block = jnp.concatenate([new[:6], row, jnp.zeros((1, HID), f32)], 0).astype(bf16)
            tiles = jnp.concatenate([block[:, EMB * j : EMB * (j + 1)] for j in range(8)], 0)
            tiles = jnp.broadcast_to(tiles.reshape(1, 2, 32, EMB), (NS // 2, 2, 32, EMB))
            served = served.at[:, SLOTS:, :].set(tiles.reshape(NS, 32, EMB))
            lists = from_groups(grads)
            for t in range(2):
                total = add_lists(me, -emb_rate * weights, all_idx, all_clash, lists, total, 0, t)
        else:
            for t in range(2):
                lists = from_groups(grads[:, t * CAP : (t + 1) * CAP])
                total = add_lists(me, -emb_rate * weights, all_idx, all_clash, lists, total, 1, t)
    mine = weights[group] * (-dense_rate / BATCH) * top_sum
    a, b, c, d = from_groups(mine)
    dense = (a + c) + (b + d)
    ends = exchange(jnp.broadcast_to(dense[6:7, :EMB][None], (NS, 1, EMB))).reshape(NS, EMB)
    return (
        total,
        dense[:6],
        ends[:DENSE],
        ends[DENSE : DENSE + 8].reshape(HID),
    )


def solution(mesh):
    in_specs = (
        P(None, "shard", None),
        P("group", None, None, "shard", None),
        P("group", None, None, "shard"),
        P("group", None, None, "shard", None),
        P("group", None, "shard", None),
        P("group", None, "shard"),
        P(),
        P("shard", None),
        P(),
        P(),
    )
    out_specs = (P(None, "shard", None), P("shard", None), P(), P())
    return jax.shard_map(whole_round, mesh=mesh, in_specs=in_specs, out_specs=out_specs, check_vma=False)
```
